16 devices in a mesh: dp: 2 (over z), tp: 8 (over y, x, core).
Axes of the slice: x: 2, y: 2, z: 2, core: 2. Of those that a mesh axis runs over, the one named last changes fastest.
Arguments:
- x_in: bfloat16 [16, 512, 6144], P('dp', 'tp'), parts along dimension 0
- ln_gamma: float32 [6144], replicated
- ln_beta: float32 [6144], replicated
- w_q: bfloat16 [6144, 6144], P(None, 'tp')
- b_q: float32 [6144], P('tp')
- w_kv: bfloat16 [6144, 256], replicated
- b_kv: float32 [256], replicated
- w_o: bfloat16 [6144, 6144], P('tp')
- b_o: float32 [6144], replicated
- grad_y: bfloat16 [16, 512, 6144], P('dp', 'tp'), parts along dimension 0
Outputs:
- output 1: bfloat16 [16, 512, 6144], P('dp', 'tp'), parts along dimension 0
- output 2: bfloat16 [16, 512, 6144], P('dp', 'tp'), parts along dimension 0
- output 3: float32 [12288], P('dp'), parts along dimension 0
- output 4: float32 [12288], P('dp'), parts along dimension 0
- output 5: float32 [12288, 6144], P('dp', 'tp'), parts along dimension 0
- output 6: float32 [12288], P(('dp', 'tp')), parts along dimension 0
- output 7: float32 [12288, 256], P('dp'), parts along dimension 0
- output 8: float32 [512], P('dp'), parts along dimension 0
- output 9: float32 [12288, 6144], P(('dp', 'tp')), parts along dimension 0
- output 10: float32 [12288], P('dp'), parts along dimension 0
There are 2 independent parts. The reference program is written for one: setup_inputs(seed, part) draws one part's arguments, and reference() takes and returns one part's arrays. A program takes and returns all parts, laid end to end along the dimension named above; an argument that names none is the same for every part.
All inputs are finite; a program needn't handle non-finite values.
Results may differ from the reference program's by a relative error of at most 0.0147521.
Values are sent between devices in bfloat16 or wider.
A program may use at most 1 GiB of HBM per device.

```python
import jax
import jax.numpy as jnp
from jax import lax

D = 6144
HEADS = 48
HEAD = 128
BATCH = 8
SEQ = 512
LN_EPS = 1e-5


def setup_inputs(seed: int = 0, part: int = 0) -> dict:
    q_width = HEADS * HEAD
    base_key = jax.random.key(seed)
    key_list = jax.random.split(base_key, 8)
    part_keys = jax.random.split(jax.random.fold_in(base_key, part), 2)
    out_gain = (SEQ / 64) ** 0.25
    x_in = jax.random.normal(part_keys[0], (BATCH, SEQ, D), jnp.float32).astype(jnp.bfloat16)
    grad_y = jax.random.normal(part_keys[1], (BATCH, SEQ, D), jnp.float32).astype(jnp.bfloat16)
    ln_gamma = 1.0 + 0.3 * jax.random.normal(key_list[0], (D,), jnp.float32)
    ln_beta = 0.3 * jax.random.normal(key_list[1], (D,), jnp.float32)
    w_q = (D ** -0.5 * jax.random.normal(key_list[2], (D, q_width), jnp.float32)).astype(jnp.bfloat16)
    b_q = 0.5 * jax.random.normal(key_list[3], (q_width,), jnp.float32)
    w_kv = (D ** -0.5 * jax.random.normal(key_list[4], (D, 2 * HEAD), jnp.float32)).astype(jnp.bfloat16)
    b_kv = 0.3 * jax.random.normal(key_list[5], (2 * HEAD,), jnp.float32)
    w_o = (out_gain * q_width ** -0.5 * jax.random.normal(key_list[6], (q_width, D), jnp.float32)).astype(jnp.bfloat16)
    b_o = 0.5 * jax.random.normal(key_list[7], (D,), jnp.float32)
    return {"x_in": x_in, "ln_gamma": ln_gamma, "ln_beta": ln_beta, "w_q": w_q, "b_q": b_q, "w_kv": w_kv, "b_kv": b_kv, "w_o": w_o, "b_o": b_o, "grad_y": grad_y}


def snap_bf16(values_in):
    return values_in.astype(jnp.bfloat16).astype(jnp.float32)


def layer_norm(x_wide, ln_gamma, ln_beta):
    centred = x_wide - jnp.mean(x_wide, axis=-1, keepdims=True)
    row_var = jnp.mean(centred * centred, axis=-1, keepdims=True)
    return centred * lax.rsqrt(row_var + LN_EPS) * ln_gamma + ln_beta


def block_forward(x_wide, ln_gamma, ln_beta, w_q, b_q, w_kv, b_kv, w_o, b_o):
    normed = snap_bf16(layer_norm(x_wide, ln_gamma, ln_beta))
    queries = snap_bf16(jnp.einsum("bsd,de->bse", normed, w_q) + b_q)
    key_val = snap_bf16(jnp.einsum("bsd,dc->bsc", normed, w_kv) + b_kv)
    key_rows = key_val[:, :, :HEAD]
    value_rows = key_val[:, :, HEAD:]
    q_heads = jnp.moveaxis(queries.reshape(BATCH, SEQ, HEADS, HEAD), 2, 0)
    positions = jnp.arange(SEQ)
    causal = positions[:, None] >= positions[None, :]

    def one_head(q_one):
        scores = jnp.einsum("bqc,bkc->bqk", q_one, key_rows) * HEAD ** -0.5
        attn_prob = snap_bf16(jax.nn.softmax(jnp.where(causal, scores, -1e30), axis=-1))
        return snap_bf16(jnp.einsum("bqk,bkc->bqc", attn_prob, value_rows))

    attended = lax.map(jax.checkpoint(one_head), q_heads)
    merged = jnp.moveaxis(attended, 0, 2).reshape(BATCH, SEQ, HEADS * HEAD)
    return x_wide + jnp.einsum("bse,ed->bsd", merged, w_o) + b_o


def reference(x_in, ln_gamma, ln_beta, w_q, b_q, w_kv, b_kv, w_o, b_o, grad_y):
    y_wide, pullback = jax.vjp(block_forward, x_in.astype(jnp.float32), ln_gamma, ln_beta, w_q.astype(jnp.float32), b_q, w_kv.astype(jnp.float32), b_kv, w_o.astype(jnp.float32), b_o)
    cotangents = pullback(grad_y.astype(jnp.float32))
    return (y_wide.astype(jnp.bfloat16), cotangents[0].astype(jnp.bfloat16), cotangents[1], cotangents[2], cotangents[3], cotangents[4], cotangents[5], cotangents[6], cotangents[7], cotangents[8])
```

```python
import jax
import jax.numpy as jnp
from jax import lax
from jax.sharding import PartitionSpec as P


LN_EPS = 1e-5
CHUNKS = 2


def norm_forward(x_loc, ln_gamma, ln_beta):
    x_wide = x_loc.astype(jnp.float32)
    centred = x_wide - jnp.mean(x_wide, axis=-1, keepdims=True)
    inv_std = lax.rsqrt(jnp.mean(centred * centred, axis=-1, keepdims=True) + LN_EPS)
    x_hat = centred * inv_std
    return x_hat, inv_std, (x_hat * ln_gamma + ln_beta).astype(jnp.bfloat16)


def norm_backward(grad_h, x_hat, inv_std, ln_gamma):
    grad_hat = grad_h * ln_gamma
    grad_in = inv_std * (grad_hat - jnp.mean(grad_hat, axis=-1, keepdims=True) - x_hat * jnp.mean(grad_hat * x_hat, axis=-1, keepdims=True))
    return grad_in, jnp.sum(grad_h * x_hat, axis=(0, 1)), jnp.sum(grad_h, axis=(0, 1))


def attn_forward(q_heads, key_rows, value_rows, causal):
    scores = jnp.einsum("bqhc,bkc->bhqk", q_heads, key_rows, preferred_element_type=jnp.float32) * q_heads.shape[-1] ** -0.5
    attn_prob = jax.nn.softmax(jnp.where(causal, scores, -1e30), axis=-1)
    prob_lo = attn_prob.astype(jnp.bfloat16)
    attended = jnp.einsum("bhqk,bkc->bqhc", prob_lo, value_rows, preferred_element_type=jnp.float32).astype(jnp.bfloat16)
    return attn_prob, prob_lo, attended


def attn_backward(grad_att, q_heads, key_rows, value_rows, attn_prob, prob_lo):
    grad_prob = jnp.einsum("bqhc,bkc->bhqk", grad_att, value_rows, preferred_element_type=jnp.float32).astype(jnp.bfloat16)
    row_dot = jnp.sum(attn_prob * grad_prob, axis=-1, keepdims=True)
    grad_score = (attn_prob * (grad_prob - row_dot) * q_heads.shape[-1] ** -0.5).astype(jnp.bfloat16)
    grad_q = jnp.einsum("bhqk,bkc->bqhc", grad_score, key_rows, preferred_element_type=jnp.float32).astype(jnp.bfloat16)
    grad_k = jnp.einsum("bhqk,bqhc->bkc", grad_score, q_heads, preferred_element_type=jnp.float32)
    grad_v = jnp.einsum("bhqk,bqhc->bkc", prob_lo, grad_att, preferred_element_type=jnp.float32)
    return grad_q, jnp.concatenate([grad_k, grad_v], axis=-1)


def solution(mesh):
    def device_block(x_loc, ln_gamma, ln_beta, w_q, b_q, w_kv, b_kv, w_o, b_o, dy_loc):
        head_dim = w_kv.shape[1] // 2
        local_heads = w_q.shape[1] // head_dim
        per = x_loc.shape[0] // CHUNKS
        local_len = x_loc.shape[1]
        cut = lambda a, c: a[c * per:(c + 1) * per]
        xs = [cut(x_loc, c) for c in range(CHUNKS)]
        dys = [cut(dy_loc, c) for c in range(CHUNKS)]
        norms = [norm_forward(xc, ln_gamma, ln_beta) for xc in xs]
        gather = lambda a: lax.all_gather(a, "tp", axis=1, tiled=True)
        h_full, dy_full = [], []
        for c in range(CHUNKS):
            dy_full.append(gather(dys[c]))
            h_full.append(gather(norms[c][2]))
        grad_bo_part = jnp.sum(dy_loc, axis=(0, 1), dtype=jnp.float32)

        y_parts, dh_parts, kv_parts = [], [], []
        grad_wq = grad_wo = grad_bq = 0.0
        for c in range(CHUNKS):
            hc, dyc = h_full[c], dy_full[c]
            if c:
                hc, _, _ = lax.optimization_barrier((hc, out_part, dh_part))
            seq_len = hc.shape[1]
            positions = jnp.arange(seq_len)
            causal = positions[:, None] >= positions[None, :]
            queries = (jnp.einsum("bsd,de->bse", hc, w_q, preferred_element_type=jnp.float32) + b_q).astype(jnp.bfloat16)
            if c:
                dyc, _ = lax.optimization_barrier((dyc, queries))
            q_heads = queries.reshape(per, seq_len, local_heads, head_dim)
            key_val = (jnp.einsum("bsd,dc->bsc", hc, w_kv, preferred_element_type=jnp.float32) + b_kv).astype(jnp.bfloat16)
            key_rows = key_val[:, :, :head_dim]
            value_rows = key_val[:, :, head_dim:]
            attn_prob, prob_lo, attended = attn_forward(q_heads, key_rows, value_rows, causal)
            merged = attended.reshape(queries.shape)
            out_part = jnp.einsum("bse,ed->bsd", merged, w_o, preferred_element_type=jnp.float32).astype(jnp.bfloat16)
            y_parts.append(lax.psum_scatter(out_part, "tp", scatter_dimension=1, tiled=True))
            grad_att = jnp.einsum("bsd,ed->bse", dyc, w_o, preferred_element_type=jnp.float32).astype(jnp.bfloat16)
            grad_q, kv_wide = attn_backward(grad_att.reshape(q_heads.shape), q_heads, key_rows, value_rows, attn_prob, prob_lo)
            grad_q = grad_q.reshape(queries.shape)
            kv_parts.append(kv_wide.astype(jnp.bfloat16))
            dh_part = jnp.einsum("bse,de->bsd", grad_q, w_q, preferred_element_type=jnp.float32).astype(jnp.bfloat16)
            dh_parts.append(lax.psum_scatter(dh_part, "tp", scatter_dimension=1, tiled=True))
            grad_wq += jnp.einsum("bsd,bse->de", hc, grad_q, preferred_element_type=jnp.float32)
            grad_wo += jnp.einsum("bse,bsd->ed", merged, dyc, preferred_element_type=jnp.float32)
            grad_bq += jnp.sum(grad_q, axis=(0, 1), dtype=jnp.float32)

        kv_sent = jnp.concatenate(kv_parts, axis=0)
        kv_got = lax.all_to_all(kv_sent, "tp", split_axis=1, concat_axis=1, tiled=True)
        kv_got = kv_got.reshape(kv_got.shape[0], -1, local_len, kv_got.shape[2])
        kv_at = jnp.sum(kv_got.astype(jnp.float32), axis=1).astype(jnp.bfloat16)
        pieces = [gather(kv_at[i:i + 2]) for i in range(0, kv_at.shape[0], 2)]
        grad_kv = jnp.concatenate(pieces, axis=0)
        grad_wkv = sum(jnp.einsum("bsd,bsc->dc", h_full[c], cut(grad_kv, c), preferred_element_type=jnp.float32) for c in range(CHUNKS))
        grad_bkv = jnp.sum(grad_kv, axis=(0, 1), dtype=jnp.float32)
        dh_kv = jnp.einsum("bsc,dc->bsd", kv_at, w_kv, preferred_element_type=jnp.float32)

        dxs = []
        gamma_part = beta_part = 0.0
        for c in range(CHUNKS):
            if c:
                dh_parts[c], _, _, _ = lax.optimization_barrier((dh_parts[c], dxs[-1], gamma_part, beta_part))
            x_hat, inv_std, _ = norms[c]
            grad_h = dh_parts[c].astype(jnp.float32) + cut(dh_kv, c)
            grad_in, g_part, b_part = norm_backward(grad_h, x_hat, inv_std, ln_gamma)
            gamma_part += g_part
            beta_part += b_part
            dxs.append((dys[c].astype(jnp.float32) + grad_in).astype(jnp.bfloat16))
        grad_x = jnp.concatenate(dxs, axis=0)
        y_parts[-1], grad_x, grad_wkv, grad_bkv = lax.optimization_barrier((y_parts[-1], grad_x, grad_wkv, grad_bkv))
        ys = [(xs[c].astype(jnp.float32) + y_parts[c].astype(jnp.float32) + b_o).astype(jnp.bfloat16) for c in range(CHUNKS)]
        smalls = lax.all_gather(jnp.stack([gamma_part, beta_part, grad_bo_part]), "tp", axis=0)
        grad_gamma, grad_beta, grad_bo = jnp.sum(smalls, axis=0)
        return (jnp.concatenate(ys, axis=0), grad_x, grad_gamma, grad_beta, grad_wq, grad_bq, grad_wkv, grad_bkv, grad_wo, grad_bo)

    return jax.shard_map(
        device_block,
        mesh=mesh,
        in_specs=(P("dp", "tp", None), P(None), P(None), P(None, "tp"), P("tp"), P(None, None), P(None), P("tp", None), P(None), P("dp", "tp", None)),
        out_specs=(P("dp", "tp", None), P("dp", "tp", None), P("dp"), P("dp"), P("dp", "tp"), P(("dp", "tp")), P("dp", None), P("dp"), P(("dp", "tp"), None), P("dp")),
        check_vma=False,
    )
```
